32 devices in a mesh: rows: 8 (over z, x), leaf: 4 (over y, core).
Axes of the slice: x: 2, y: 2, z: 4, core: 2. Of those that a mesh axis runs over, the one named last changes fastest.
Arguments:
- right_sides: float32 [65536, 128], P(('rows', 'leaf')), may hold values from -30 to 30
- near_blocks: bfloat16 [2, 128, 512, 512], P(None, ('rows', 'leaf')), may hold values from -1 to 2.4
- leaf_bases: bfloat16 [2, 128, 2, 512, 128], P(None, ('rows', 'leaf')), may hold values from -1.5 to 1.5
- local_factors: bfloat16 [2, 224, 3, 128, 128], P(None, ('rows', 'leaf')), may hold values from -1.7 to 1.7
- upper_factors: bfloat16 [2, 32, 3, 3, 128, 128], P(None, ('rows', 'leaf')), may hold values from -1.7 to 1.7, as said below
- top_couplings: bfloat16 [2, 2, 128, 128], replicated, may hold values from -0.5 to 0.5
Outputs:
- solution: float32 [65536, 128], P(('rows', 'leaf'))
- residual_norms: float32 [3, 128], replicated
The draws below stay inside these ranges and needn't reach their ends.
Inputs may be any that keep to these rules, and one draw needn't show every extreme that they name: upper_factors[s, d, h] is the same for all devices d with the same d // 2 ** (h + 1): the factors of the node h + 1 levels above device d's own node.
All inputs are finite; a program needn't handle non-finite values.
Results may differ from the reference program's by a relative error of at most 0.00095.
Values sent between devices are 32-bit elements; how exact they have to be, the bound alone decides.
A program may use at most 128 MiB of HBM per device.

```python
import math
import jax
import jax.numpy as jnp
from jax import lax

LEAF = 512
RANK = 128
RHS = 128
LEAF_DEV = 4
STEPS = 3
UPPER = 3
NLEAVES = 128
ORDER = 65536
N_ROWS = 8
N_LEAF = 4


def clipped(key_value, shape):
    return jnp.clip(jax.random.normal(key_value, shape, jnp.float32), -6.0, 6.0)


def node_factors(key_value, node_count):
    keys = jax.random.split(key_value, 6)
    shape = (node_count, RANK, RANK)
    spread = RANK ** (-0.5)
    identity_matrix = jnp.eye(RANK, dtype=jnp.float32)
    up_transfer = (identity_matrix + 0.3 * spread * clipped(keys[0], shape)) * 0.7071
    down_transfer = (identity_matrix + 0.3 * spread * clipped(keys[1], shape)) * 0.96
    coupling = 0.1 * spread * clipped(keys[2], shape)
    operator_part = jnp.stack([up_transfer, down_transfer, coupling], axis=1)
    inverse_part = jnp.stack([up_transfer + 0.05 * spread * clipped(keys[3], shape), down_transfer + 0.05 * spread * clipped(keys[4], shape), 0.02 * spread * clipped(keys[5], shape) - coupling], axis=1)
    return (operator_part, inverse_part)


def draw_right_sides(key, part):
    first_key = jax.random.fold_in(jax.random.fold_in(key, 606), 0)
    growth = jnp.exp(math.log(3.0) * jnp.arange(ORDER, dtype=jnp.float32) / ORDER)
    return clipped(first_key, (ORDER, RHS)) * growth[:, None]


def draw_near_blocks(key, part):
    keys = jax.random.split(jax.random.fold_in(key, 404), 3)
    diagonal_gain = jax.random.uniform(keys[0], (NLEAVES, LEAF), jnp.float32, 0.8, 1.25)
    coupling = clipped(keys[1], (NLEAVES, LEAF, LEAF)) * (0.2 * LEAF ** (-0.5))
    noise_term = clipped(keys[2], (NLEAVES, LEAF, LEAF)) * (0.45 * LEAF ** (-0.5))
    identity_matrix = jnp.eye(LEAF, dtype=jnp.float32)
    operator_block = identity_matrix * diagonal_gain[:, :, None] + coupling
    inverse_gain = 1.0 / diagonal_gain
    inverse_block = identity_matrix * inverse_gain[:, :, None] - inverse_gain[:, :, None] * coupling * inverse_gain[:, None, :] + noise_term
    return jnp.stack([operator_block, inverse_block]).astype(jnp.bfloat16)


def draw_leaf_bases(key, part):
    first_key, second_key = jax.random.split(jax.random.fold_in(key, 505))
    shape = (NLEAVES, 2, LEAF, RANK)
    operator_bases = clipped(first_key, shape) * LEAF ** (-0.5)
    inverse_bases = operator_bases + 0.1 * clipped(second_key, shape) * LEAF ** (-0.5)
    return jnp.stack([operator_bases, inverse_bases]).astype(jnp.bfloat16)


def draw_local_factors(key, part):
    operator_part, inverse_part = node_factors(jax.random.fold_in(key, 101), (2 * LEAF_DEV - 1) * N_ROWS * N_LEAF)
    return jnp.stack([operator_part, inverse_part]).astype(jnp.bfloat16)


def draw_upper_factors(key, part):
    operator_levels = []
    inverse_levels = []
    for height in range(1, UPPER + 1):
        node_count = N_ROWS * N_LEAF // 2 ** height
        operator_part, inverse_part = node_factors(jax.random.fold_in(jax.random.fold_in(key, 202), height), node_count)
        operator_levels.append(jnp.repeat(operator_part, 2 ** height, axis=0))
        inverse_levels.append(jnp.repeat(inverse_part, 2 ** height, axis=0))
    return jnp.stack([jnp.stack(operator_levels, axis=1), jnp.stack(inverse_levels, axis=1)]).astype(jnp.bfloat16)


def draw_top_couplings(key, part):
    first_key, second_key = jax.random.split(jax.random.fold_in(key, 303))
    spread = RANK ** (-0.5)
    coupling = 0.1 * spread * clipped(first_key, (2, RANK, RANK))
    inverse_coupling = 0.02 * spread * clipped(second_key, (2, RANK, RANK)) - coupling
    return jnp.stack([coupling, inverse_coupling]).astype(jnp.bfloat16)


def setup_inputs(seed: int = 0) -> dict:
    seeds = jax.random.split(jax.random.key(seed), 7)
    return {
        "right_sides": draw_right_sides(jax.random.fold_in(seeds[6], 71), 0),
        "near_blocks": draw_near_blocks(jax.random.fold_in(seeds[6], 71), 0),
        "leaf_bases": draw_leaf_bases(jax.random.fold_in(seeds[6], 71), 0),
        "local_factors": draw_local_factors(jax.random.fold_in(seeds[6], 71), 0),
        "upper_factors": draw_upper_factors(jax.random.fold_in(seeds[6], 71), 0),
        "top_couplings": draw_top_couplings(jax.random.fold_in(seeds[6], 71), 0),
    }


HIGHEST = lax.Precision.HIGHEST


def split_pair(values):
    upper_half = lax.optimization_barrier(values.astype(jnp.bfloat16))
    lower_half = (values - upper_half.astype(jnp.float32)).astype(jnp.bfloat16)
    return (upper_half, lower_half)


def sibling_of(values):
    shaped = values.reshape((values.shape[0] // 2, 2) + values.shape[1:])
    return shaped[:, ::-1].reshape(values.shape)


def level_tables(local_factors, upper_factors, member):
    per_device = local_factors[member].reshape(N_ROWS * N_LEAF, 2 * LEAF_DEV - 1, 3, RANK, RANK)
    tables = []
    offset = 0
    node_count = LEAF_DEV
    while node_count >= 1:
        factor_block = per_device[:, offset:offset + node_count]
        tables.append(factor_block.reshape(-1, 3, RANK, RANK).astype(jnp.float32))
        offset = offset + node_count
        node_count = node_count // 2
    for height in range(1, UPPER + 1):
        tables.append(upper_factors[member, ::2 ** height, height - 1].astype(jnp.float32))
    return tables


def near_and_coefficient(items):
    square, column_basis, stacked_pieces = items
    near_field = jnp.zeros((square.shape[0], stacked_pieces.shape[2]), jnp.float32)
    coefficient = jnp.zeros((column_basis.shape[1], stacked_pieces.shape[2]), jnp.float32)
    for piece_index in range(stacked_pieces.shape[0]):
        piece_value = stacked_pieces[piece_index]
        near_field = near_field + jnp.dot(square, piece_value, preferred_element_type=jnp.float32)
        coefficient = coefficient + jnp.dot(column_basis.T, piece_value, preferred_element_type=jnp.float32)
    return near_field, coefficient


def far_product(items):
    row_basis, stacked_far = items
    result = jnp.zeros((row_basis.shape[0], stacked_far.shape[2]), jnp.float32)
    for piece_index in range(stacked_far.shape[0]):
        result = result + jnp.dot(row_basis, stacked_far[piece_index], preferred_element_type=jnp.float32)
    return result


def apply_tree(near_set, basis_set, tables, top_pair, pieces, split_far):
    stacked = jnp.stack(pieces, axis=1)
    near_field, coefficient = lax.map(near_and_coefficient, (near_set, basis_set[:, 1], stacked))
    lower_list = []
    for factor_table in tables:
        lower_list.append(coefficient)
        projected = jnp.einsum("nab,nac->nbc", factor_table[:, 0], coefficient, precision=HIGHEST)
        coefficient = projected[0::2] + projected[1::2]
    far_field = jnp.einsum("nab,nbc->nac", top_pair.astype(jnp.float32), sibling_of(coefficient), precision=HIGHEST)
    for factor_table, lower_value in zip(tables[::-1], lower_list[::-1]):
        far_field = jnp.einsum("nab,nbc->nac", factor_table[:, 1], jnp.repeat(far_field, 2, axis=0), precision=HIGHEST) + jnp.einsum("nab,nbc->nac", factor_table[:, 2], sibling_of(lower_value), precision=HIGHEST)
    if split_far:
        far_parts = split_pair(far_field)
    else:
        far_parts = (far_field.astype(jnp.bfloat16),)
    return near_field + lax.map(far_product, (basis_set[:, 0], jnp.stack(far_parts, axis=1)))


def reference(right_sides, near_blocks, leaf_bases, local_factors, upper_factors, top_couplings):
    leaves = right_sides.shape[0] // LEAF
    right_side = right_sides.reshape(leaves, LEAF, RHS)
    tables_operator = level_tables(local_factors, upper_factors, 0)
    tables_inverse = level_tables(local_factors, upper_factors, 1)

    def operator(values):
        return apply_tree(near_blocks[0], leaf_bases[0], tables_operator, top_couplings[0], split_pair(values), True)

    def inverse(values):
        return apply_tree(near_blocks[1], leaf_bases[1], tables_inverse, top_couplings[1], (values.astype(jnp.bfloat16),), False)

    solution = inverse(right_side)
    norm_list = []
    for refine_step in range(STEPS):
        residual = right_side - operator(solution)
        norm_list.append(jnp.sum(residual * residual, axis=(0, 1)))
        solution = solution + inverse(residual)
    return (solution.reshape(right_sides.shape[0], RHS), jnp.stack(norm_list))
```

```python
import functools
import jax
import jax.numpy as jnp
from jax import lax
from jax.experimental import pallas as pl
from jax.experimental.pallas import tpu as pltpu
from jax.sharding import PartitionSpec as P

STEPS = 3
F32 = jnp.float32
BF16 = jnp.bfloat16
NT = (((1,), (1,)), ((), ()))


def dot(a, b):
    return jnp.dot(a, b, preferred_element_type=F32)


def split(v):
    hi = v.astype(BF16)
    lo = (v - hi.astype(F32)).astype(BF16)
    return hi, lo


def wide(v):
    return jnp.concatenate(split(v), axis=1)


def tall(v):
    return jnp.concatenate(split(v), axis=0)


def fold_cols(v):
    n = v.shape[1] // 2
    return v[:, :n] + v[:, n:]


def fold_rows(v):
    n = v.shape[0] // 2
    return v[:n] + v[n:]


def kernel(
    bits_leaf, bits_rows,
    rhs_hbm, near_hbm, bases_hbm, local_hbm, upper_hbm, top_hbm,
    x_ref, norm_ref,
    b_ref, r_ref, near, bases, local, upper, top,
    vt, pt, tt, cb, pre, nrm,
    send_a, send_b, recv_a, recv_b, send_n, recv_n, sib_full, full,
    load_sem, send_sem, recv_sem,
):
    leaves = near.shape[1]
    rank = bases.shape[4]
    levels = bits_leaf + bits_rows
    last = levels - 1
    root = 2 * leaves - 2
    leaf = lax.axis_index("leaf")
    rows = lax.axis_index("rows")
    half = x_ref.shape[2] // 2
    mine = pl.multiple_of(leaf % 2 * half, half)
    other = pl.multiple_of((1 - leaf % 2) * half, half)
    top_pos = rows // 2 ** (bits_rows - 1)

    def partner(level):
        if level < bits_leaf:
            d = 2**level
            flip = leaf + d - 2 * d * (leaf // d % 2)
            return (rows, flip)
        d = 2 ** (level - bits_leaf)
        flip = rows + d - 2 * d * (rows // d % 2)
        return (flip, leaf)

    def load(src, dst, index):
        return pltpu.make_async_copy(src, dst, load_sem.at[index])

    loads = {}
    order = [("rhs", rhs_hbm, b_ref), ("res", rhs_hbm, r_ref)]
    for s in (1, 0):
        order += [
            (("bases", s), bases_hbm.at[s], bases.at[s]),
            (("local", s), local_hbm.at[s], local.at[s]),
            (("upper", s), upper_hbm.at[s, 0], upper.at[s]),
            (("top", s), top_hbm.at[s], top.at[s]),
            (("near", s), near_hbm.at[s], near.at[s]),
        ]
    for index, (name, src, dst) in enumerate(order):
        loads[name] = load(src, dst, index)
        loads[name].start()

    barrier = pltpu.get_barrier_semaphore()
    for level in range(levels):
        pl.semaphore_signal(
            barrier, inc=1, device_id=partner(level), device_id_type=pl.DeviceIdType.MESH
        )

    def setup_up(s):
        loads["bases", s].wait()
        loads["local", s].wait()
        for i in range(leaves):
            vt[s, i] = bases[s, i, 1].astype(F32).T.astype(BF16)
        for p in range(leaves - 1):
            pair = [local[s, 2 * p + j, 0].astype(F32).T.astype(BF16) for j in range(2)]
            pt[s, p] = jnp.concatenate(pair, axis=1)

    def setup_down(s):
        loads["upper", s].wait()
        loads["top", s].wait()
        chain = None
        for level in range(1, levels):
            coupling = top[s, top_pos] if level == last else upper[s, level - 1, 2]
            if chain is None:
                product = coupling.astype(F32)
            else:
                product = fold_rows(dot(tall(chain), coupling))
            tt[s, level] = wide(product.T)
            if level < last:
                q = upper[s, level - 1, 1]
                chain = q.astype(F32) if chain is None else fold_rows(dot(tall(chain), q))

    def remote(s, index, src, dst, level):
        return pltpu.make_async_remote_copy(
            src_ref=src,
            dst_ref=dst,
            send_sem=send_sem.at[s, index],
            recv_sem=recv_sem.at[s, index],
            device_id=partner(level),
            device_id_type=pl.DeviceIdType.MESH,
        )

    def apply(s, norms, hooks):
        def pieces(i):
            return wide(x_ref[i]) if s == 0 else r_ref[i].astype(BF16)

        def fold(v):
            return fold_cols(v) if s == 0 else v

        def near_leaf(i):
            value = fold(dot(near[s, i], pieces(i)))
            if s == 0:
                r_ref[i] = b_ref[i] - value
            else:
                x_ref[i] = x_ref[i] + value

        def couple(n):
            sibling = n + 1 - 2 * (n % 2)
            pre[n] = fold_cols(dot(local[s, n, 2], cb[sibling]))

        for i in range(leaves):
            cb[i] = wide(fold(dot(vt[s, i], pieces(i))))
        for p in range(leaves - 1):
            stacked = jnp.concatenate([cb[2 * p], cb[2 * p + 1]], axis=0)
            coefficient = fold_cols(dot(pt[s, p], stacked))
            if p < leaves - 2:
                cb[leaves + p] = wide(coefficient)
        started = []

        def start(index, src, dst, level):
            copy = remote(s, index, src, dst, level)
            copy.start()
            started.append(copy)
            return copy

        full[s] = fold_rows(dot(tall(coefficient.T), local[s, root, 0]))
        sib_full[s, 0] = coefficient
        work = list(range(leaves))
        hooks = list(hooks)
        total = nrm[0] if norms is not None else None
        far = None
        previous_b = None
        for level in range(levels):
            base = 3 * level
            if level == 0:
                copy_a = start(base, full.at[s, pl.ds(other, half)], recv_a.at[s, 0], 0)
            else:
                if level == last:
                    send_a[s, level] = value
                else:
                    send_a[s, level] = fold_rows(dot(tall(value), upper[s, level - 1, 0]))
                copy_a = start(base, send_a.at[s, level], recv_a.at[s, level], level)
            if norms is not None:
                send_n[level] = total
                copy_n = start(base + 1, send_n.at[level], recv_n.at[level], level)
            copy_b = None
            if level == 0:
                copy_b = start(base + 2, sib_full.at[s, 0], sib_full.at[s, 1], 0)
            elif level < last:
                send_b[s, level] = value
                copy_b = start(base + 2, send_b.at[s, level], recv_b.at[s, level], level)
            if hooks:
                hooks.pop(0)()
            if work:
                near_leaf(work.pop(0))
            if level == last:
                while work:
                    near_leaf(work.pop(0))
                while hooks:
                    hooks.pop(0)()
            if level == 1:
                for n in range(root):
                    couple(n)
            if previous_b is not None:
                previous_b.wait_recv()
                if level == 1:
                    root_pre = fold_cols(dot(local[s, root, 2], wide(sib_full[s, 1])))
                else:
                    term = across(s, recv_b[s, level - 1], level - 1)
                    far = term if far is None else far + term
            previous_b = copy_b
            copy_a.wait_recv()
            if level == 0:
                value = full[s, pl.ds(mine, half)] + recv_a[s, 0]
            elif level < last:
                value = send_a[s, level] + recv_a[s, level]
            if norms is not None:
                copy_n.wait_recv()
                total = total + recv_n[level]
        term = across(s, recv_a[s, last], last)
        far = term if far is None else far + term
        sib_full[s, 2, pl.ds(mine, half)] = far
        copy = start(
            3 * levels,
            sib_full.at[s, 2, pl.ds(mine, half)],
            sib_full.at[s, 2, pl.ds(mine, half)],
            0,
        )
        if norms is not None:
            nrm[norms] = total
        copy.wait_recv()
        far_t = tall(sib_full[s, 2])
        field = {}
        field[root] = (
            fold_cols(
                lax.dot_general(local[s, root, 1], far_t, NT, preferred_element_type=F32)
            )
            + root_pre
        )
        for n in range(root - 1, -1, -1):
            parent = leaves + n // 2
            if not isinstance(field[parent], tuple):
                field[parent] = (wide(field[parent]),)
            field[n] = fold_cols(dot(local[s, n, 1], field[parent][0])) + pre[n]
        partial = None
        for i in range(leaves):
            if s == 0:
                out = r_ref[i] - fold_cols(dot(bases[s, i, 0], wide(field[i])))
                r_ref[i] = out
                square = jnp.sum((out * out).reshape(-1, 8, out.shape[1]), axis=0)
                partial = square if partial is None else partial + square
            else:
                x_ref[i] = x_ref[i] + dot(bases[s, i, 0], field[i].astype(BF16))
        if s == 0:
            nrm[0] = partial
        for copy in started:
            copy.wait_send()

    def across(s, value, level):
        out = dot(tall(value), tt[s, level])
        n, m = out.shape[0] // 2, out.shape[1] // 2
        return out[:n, :m] + (out[:n, m:] + out[n:, :m])

    setup_up(1)
    x_ref[...] = jnp.zeros(x_ref.shape, F32)
    loads["rhs"].wait()
    loads["res"].wait()
    pl.semaphore_wait(barrier, levels)

    def first():
        setup_down(1)
        loads["near", 1].wait()

    def second():
        setup_up(0)

    def third():
        setup_down(0)
        loads["near", 0].wait()

    apply(1, None, [first, second, third])

    def step(k, carry):
        apply(0, None, [])
        apply(1, k + 1, [])
        return carry

    lax.fori_loop(0, STEPS, step, 0)
    for k in range(STEPS):
        norm_ref[pl.ds(k, 1)] = jnp.sum(nrm[k + 1], axis=0, keepdims=True)


def body(right_sides, near_blocks, leaf_bases, local_factors, upper_factors, top_couplings):
    bits_leaf = lax.axis_size("leaf").bit_length() - 1
    bits_rows = lax.axis_size("rows").bit_length() - 1
    levels = bits_leaf + bits_rows
    leaves, size = near_blocks.shape[1], near_blocks.shape[2]
    rank = leaf_bases.shape[4]
    columns = right_sides.shape[1]
    half = columns // 2
    nodes = local_factors.shape[1]
    heights = upper_factors.shape[2]
    vmem = pltpu.VMEM
    out, norms = pl.pallas_call(
        functools.partial(kernel, bits_leaf, bits_rows),
        out_shape=(
            jax.ShapeDtypeStruct((leaves, size, columns), F32),
            jax.ShapeDtypeStruct((STEPS, columns), F32),
        ),
        in_specs=[pl.BlockSpec(memory_space=pl.ANY)] * 6,
        out_specs=(pl.BlockSpec(memory_space=vmem), pl.BlockSpec(memory_space=vmem)),
        scratch_shapes=[
            vmem((leaves, size, columns), F32),
            vmem((leaves, size, columns), F32),
            vmem((2, leaves, size, size), BF16),
            vmem((2, leaves, 2, size, rank), BF16),
            vmem((2, nodes, 3, rank, rank), BF16),
            vmem((2, heights, 3, rank, rank), BF16),
            vmem((2, 2, rank, rank), BF16),
            vmem((2, leaves, rank, size), BF16),
            vmem((2, leaves - 1, rank, 2 * rank), BF16),
            vmem((2, levels, rank, 2 * rank), BF16),
            vmem((nodes - 1, rank, 2 * columns), BF16),
            vmem((nodes - 1, rank, columns), F32),
            vmem((STEPS + 1, 8, columns), F32),
            vmem((2, levels, half, rank), F32),
            vmem((2, levels, half, rank), F32),
            vmem((2, levels, half, rank), F32),
            vmem((2, levels, half, rank), F32),
            vmem((levels, 8, columns), F32),
            vmem((levels, 8, columns), F32),
            vmem((2, 3, rank, columns), F32),
            vmem((2, columns, rank), F32),
            pltpu.SemaphoreType.DMA((12,)),
            pltpu.SemaphoreType.DMA((2, 3 * levels + 1)),
            pltpu.SemaphoreType.DMA((2, 3 * levels + 1)),
        ],
        compiler_params=pltpu.CompilerParams(
            collective_id=0, has_side_effects=True, vmem_limit_bytes=48 * 1024 * 1024
        ),
    )(
        right_sides.reshape(leaves, size, columns),
        near_blocks,
        leaf_bases,
        local_factors,
        upper_factors,
        top_couplings,
    )
    return out.reshape(-1, columns), norms


def solution(mesh):
    placed = (
        P(("rows", "leaf"), None),
        P(None, ("rows", "leaf"), None, None),
        P(None, ("rows", "leaf"), None, None, None),
        P(None, ("rows", "leaf"), None, None, None),
        P(None, ("rows", "leaf"), None, None, None, None),
        P(),
    )
    return jax.shard_map(
        body,
        mesh=mesh,
        in_specs=placed,
        out_specs=(P(("rows", "leaf"), None), P()),
        check_vma=False,
    )
```

```python
import functools
import jax
import jax.numpy as jnp
from jax import lax
from jax.experimental import pallas as pl
from jax.experimental.pallas import tpu as pltpu
from jax.sharding import PartitionSpec as P

STEPS = 3
F32 = jnp.float32
BF16 = jnp.bfloat16
NT = (((1,), (1,)), ((), ()))


def dot(a, b):
    return jnp.dot(a, b, preferred_element_type=F32)


def split(v):
    hi = v.astype(BF16)
    lo = (v - hi.astype(F32)).astype(BF16)
    return hi, lo


def wide(v):
    return jnp.concatenate(split(v), axis=1)


def tall(v):
    return jnp.concatenate(split(v), axis=0)


def fold_cols(v):
    n = v.shape[1] // 2
    return v[:, :n] + v[:, n:]


def fold_rows(v):
    n = v.shape[0] // 2
    return v[:n] + v[n:]


def combine(out):
    n, m = out.shape[0] // 2, out.shape[1] // 2
    return out[:n, :m] + (out[:n, m:] + out[n:, :m])


def group_bits(levels):
    return min(3, levels - 1)


def kernel(
    bits_leaf, bits_rows,
    rhs_hbm, near_hbm, bases_hbm, local_hbm, upper_hbm, top_hbm,
    x_ref, norm_ref,
    b_ref, r_ref, near, bases, local, upper, top,
    vt, pt, tt, et, jt, cb, pre, nrm,
    w_send, w_recv, high_a, high_b, got_a, got_b, plane,
    send_a, send_b, recv_a, recv_b, sib_full, full,
    load_sem, send_sem, recv_sem,
):
    leaves = near.shape[1]
    levels = bits_leaf + bits_rows
    last = levels - 1
    bits = group_bits(levels)
    group = 2**bits
    root = 2 * leaves - 2
    leaf = lax.axis_index("leaf")
    rows = lax.axis_index("rows")
    columns = x_ref.shape[2]
    half = columns // 2
    cut = columns // group
    mine = pl.multiple_of(leaf % 2 * half, half)
    other = pl.multiple_of((1 - leaf % 2) * half, half)
    top_pos = rows // 2 ** (bits_rows - 1)

    def flipped(value, mask):
        for bit in range(mask.bit_length()):
            d = 2**bit
            if mask & d:
                value = value + d - 2 * d * (value // d % 2)
        return value

    def device(mask):
        leaf_mask = mask % 2**bits_leaf
        return (flipped(rows, mask // 2**bits_leaf), flipped(leaf, leaf_mask))

    def member(place):
        row, column = place
        if bits <= bits_leaf:
            return column % group
        return column + 2**bits_leaf * (row % 2 ** (bits - bits_leaf))

    me = member((rows, leaf))
    my_rows = pl.multiple_of(me * cut, cut)

    def load(src, dst, index):
        return pltpu.make_async_copy(src, dst, load_sem.at[index])

    loads = {}
    order = []
    for s in (1, 0):
        order += [
            (("local", s), local_hbm.at[s], local.at[s]),
            (("upper", s), upper_hbm.at[s, 0], upper.at[s]),
            (("bases", s), bases_hbm.at[s], bases.at[s]),
        ]
        if s == 1:
            order += [("res", rhs_hbm, r_ref)]
        order += [
            (("near", s), near_hbm.at[s], near.at[s]),
            (("top", s), top_hbm.at[s], top.at[s]),
        ]
        if s == 1:
            order += [("rhs", rhs_hbm, b_ref)]
    for index, (name, src, dst) in enumerate(order):
        loads[name] = load(src, dst, index)
        loads[name].start()

    barrier = pltpu.get_barrier_semaphore()
    partners = list(range(1, group)) + [2**level for level in range(bits, levels)]
    for mask in partners:
        pl.semaphore_signal(
            barrier, inc=1, device_id=device(mask), device_id_type=pl.DeviceIdType.MESH
        )

    def chain(s, which):
        product = upper[s, bits - 2, which].astype(F32)
        for index in range(bits - 3, -1, -1):
            product = fold_cols(dot(upper[s, index, which], wide(product)))
        node = {root: fold_cols(dot(local[s, root, which], wide(product)))}
        for n in range(root - 1, -1, -1):
            parent = leaves + n // 2
            node[n] = fold_cols(dot(local[s, n, which], wide(node[parent])))
        return [node[i] for i in range(leaves)]

    def setup_chain(s):
        loads["local", s].wait()
        loads["upper", s].wait()
        et[s] = tall(jnp.concatenate([v.T for v in chain(s, 0)], axis=1))

    def setup_up(s):
        loads["bases", s].wait()
        for i in range(leaves):
            vt[s, i] = bases[s, i, 1].astype(F32).T.astype(BF16)

    def setup_pairs(s):
        for p in range(leaves - 1):
            pair = [local[s, 2 * p + j, 0].astype(F32).T.astype(BF16) for j in range(2)]
            pt[s, p] = jnp.concatenate(pair, axis=1)

    def setup_couplings(s):
        loads["top", s].wait()
        for first, stop in ((1, bits), (bits, levels)):
            product = None
            for level in range(first, stop):
                coupling = top[s, top_pos] if level == last else upper[s, level - 1, 2]
                if product is None:
                    value = coupling.astype(F32)
                else:
                    value = fold_rows(dot(tall(product), coupling))
                tt[s, level] = wide(value.T)
                if level + 1 < stop:
                    q = upper[s, level - 1, 1]
                    product = q.astype(F32) if product is None else fold_rows(dot(tall(product), q))

    def setup_down(s):
        jt[s] = tall(jnp.concatenate(chain(s, 1), axis=0))

    def across(s, value, level):
        return combine(dot(tall(value), tt[s, level]))

    def apply(s, norms, hooks):
        started = []
        counter = [0]

        def start(src, dst, mask):
            index = counter[0]
            counter[0] += 1
            copy = pltpu.make_async_remote_copy(
                src_ref=src,
                dst_ref=dst,
                send_sem=send_sem.at[s, index],
                recv_sem=recv_sem.at[s, index],
                device_id=device(mask),
                device_id_type=pl.DeviceIdType.MESH,
            )
            copy.start()
            started.append(copy)
            return copy

        def pieces(i):
            return wide(x_ref[i]) if s == 0 else r_ref[i].astype(BF16)

        def fold(v):
            return fold_cols(v) if s == 0 else v

        def near_leaf(i):
            value = fold(dot(near[s, i], pieces(i)))
            if s == 0:
                r_ref[i] = b_ref[i] - value
            else:
                x_ref[i] = x_ref[i] + value

        def couple(n):
            sibling = n + 1 - 2 * (n % 2)
            pre[n] = fold_cols(dot(local[s, n, 2], cb[sibling]))

        field = {}

        def inner():
            for p in range(leaves - 1):
                stacked = jnp.concatenate([cb[2 * p], cb[2 * p + 1]], axis=0)
                coefficient = fold_cols(dot(pt[s, p], stacked))
                if p < leaves - 2:
                    cb[leaves + p] = wide(coefficient)
            full[s] = fold_rows(dot(tall(coefficient.T), local[s, root, 0]))
            sib_full[s, 0] = coefficient
            copy_a = start(full.at[s, pl.ds(other, half)], recv_a.at[s, 0], 1)
            copies_b = [start(sib_full.at[s, 0], sib_full.at[s, 1], 1)]
            yield
            for level in range(1, bits):
                copy_a.wait_recv()
                if level == 1:
                    value = full[s, pl.ds(mine, half)] + recv_a[s, 0]
                else:
                    value = send_a[s, level - 1] + recv_a[s, level - 1]
                if level < bits - 1:
                    send_a[s, level] = fold_rows(dot(tall(value), upper[s, level - 1, 0]))
                    copy_a = start(send_a.at[s, level], recv_a.at[s, level], 2**level)
                send_b[s, level] = value
                copies_b.append(start(send_b.at[s, level], recv_b.at[s, level], 2**level))
                if level == 1:
                    for n in range(root):
                        couple(n)
                    copies_b[0].wait_recv()
                    root_pre = fold_cols(dot(local[s, root, 2], wide(sib_full[s, 1])))
                yield
            far = None
            for level in range(1, bits):
                copies_b[level].wait_recv()
                term = across(s, recv_b[s, level], level)
                far = term if far is None else far + term
            sib_full[s, 2, pl.ds(mine, half)] = far
            copy = start(
                sib_full.at[s, 2, pl.ds(mine, half)], sib_full.at[s, 2, pl.ds(mine, half)], 1
            )
            yield
            copy.wait_recv()
            far_t = tall(sib_full[s, 2])
            product = lax.dot_general(local[s, root, 1], far_t, NT, preferred_element_type=F32)
            field[root] = fold_cols(product) + root_pre
            for n in range(root - 1, -1, -1):
                parent = leaves + n // 2
                field[n] = fold_cols(dot(local[s, n, 1], wide(field[parent]))) + pre[n]
            yield

        for i in range(leaves):
            cb[i] = wide(fold(dot(vt[s, i], pieces(i))))
        stacked = jnp.concatenate([cb[i] for i in range(leaves)], axis=0)
        outer_t = combine(dot(et[s], stacked)).T
        size = cut if norms is None else cut + 8
        for j in range(group):
            w_send[s, j, :cut] = outer_t[j * cut : (j + 1) * cut]
            if norms is not None:
                w_send[s, j, cut:] = nrm[0]
        copies_w = []
        for e in range(group - 1, 0, -1):
            copies_w.append(
                start(
                    w_send.at[s, member(device(e)), pl.ds(0, size)],
                    w_recv.at[s, e, pl.ds(0, size)],
                    e,
                )
            )
        steps = inner()
        work = list(range(leaves))
        hooks = list(hooks)

        def fill(everything=False):
            if hooks:
                hooks.pop(0)()
            next(steps, None)
            while work:
                near_leaf(work.pop(0))
                if not everything:
                    break

        fill()
        fill()
        for copy in copies_w:
            copy.wait_recv()
        value = w_send[s, me, pl.ds(0, size)]
        for e in range(1, group):
            value = value + w_recv[s, e, pl.ds(0, size)]
        far = None
        for level in range(bits, levels):
            coefficient = value[:cut]
            if level == last:
                high_a[s, level, :cut] = coefficient
            else:
                high_a[s, level, :cut] = fold_rows(
                    dot(tall(coefficient), upper[s, level - 1, 0])
                )
            if norms is not None:
                high_a[s, level, cut:] = value[cut:]
            copy_a = start(
                high_a.at[s, level, pl.ds(0, size)], got_a.at[s, level, pl.ds(0, size)], 2**level
            )
            if level < last:
                high_b[s, level] = coefficient
                copy_b = start(high_b.at[s, level], got_b.at[s, level], 2**level)
            fill(level == last)
            if level == last:
                while hooks:
                    hooks.pop(0)()
            copy_a.wait_recv()
            if level == last:
                term = across(s, got_a[s, level, pl.ds(0, cut)], level)
                if norms is not None:
                    nrm[norms] = value[cut:] + got_a[s, level, pl.ds(cut, 8)]
            else:
                value = high_a[s, level, pl.ds(0, size)] + got_a[s, level, pl.ds(0, size)]
                copy_b.wait_recv()
                term = across(s, got_b[s, level], level)
            far = term if far is None else far + term
        plane[s, pl.ds(my_rows, cut)] = far
        copies_f = []
        for e in range(group - 1, 0, -1):
            piece = plane.at[s, pl.ds(my_rows, cut)]
            copies_f.append(start(piece, piece, e))
        for _ in steps:
            pass
        for copy in copies_f:
            copy.wait_recv()
        outer = combine(
            lax.dot_general(jt[s], tall(plane[s]), NT, preferred_element_type=F32)
        )
        rank = plane.shape[2]
        partial = None
        for i in range(leaves):
            total = field[i] + outer[i * rank : (i + 1) * rank]
            if s == 0:
                out = r_ref[i] - fold_cols(dot(bases[s, i, 0], wide(total)))
                r_ref[i] = out
                square = jnp.sum((out * out).reshape(-1, 8, out.shape[1]), axis=0)
                partial = square if partial is None else partial + square
            else:
                x_ref[i] = x_ref[i] + dot(bases[s, i, 0], total.astype(BF16))
        if s == 0:
            nrm[0] = partial
        for copy in started:
            copy.wait_send()

    setup_chain(1)
    setup_up(1)
    x_ref[...] = jnp.zeros(x_ref.shape, F32)
    loads["res"].wait()
    pl.semaphore_wait(barrier, len(partners))

    def first():
        setup_pairs(1)
        loads["near", 1].wait()

    def second():
        setup_couplings(1)
        setup_down(1)

    def third():
        setup_chain(0)
        setup_up(0)
        setup_pairs(0)

    def fourth():
        setup_couplings(0)
        setup_down(0)
        loads["near", 0].wait()
        loads["rhs"].wait()

    apply(1, None, [first, second, third, fourth])

    def step(k, carry):
        apply(0, None, [])
        apply(1, k + 1, [])
        return carry

    lax.fori_loop(0, STEPS, step, 0)
    for k in range(STEPS):
        norm_ref[pl.ds(k, 1)] = jnp.sum(nrm[k + 1], axis=0, keepdims=True)


def body(right_sides, near_blocks, leaf_bases, local_factors, upper_factors, top_couplings):
    bits_leaf = lax.axis_size("leaf").bit_length() - 1
    bits_rows = lax.axis_size("rows").bit_length() - 1
    levels = bits_leaf + bits_rows
    leaves, size = near_blocks.shape[1], near_blocks.shape[2]
    rank = leaf_bases.shape[4]
    columns = right_sides.shape[1]
    half = columns // 2
    bits = group_bits(levels)
    group = 2**bits
    cut = columns // group
    copies = 2 * (group - 1) + 2 * levels
    nodes = local_factors.shape[1]
    heights = upper_factors.shape[2]
    vmem = pltpu.VMEM
    out, norms = pl.pallas_call(
        functools.partial(kernel, bits_leaf, bits_rows),
        out_shape=(
            jax.ShapeDtypeStruct((leaves, size, columns), F32),
            jax.ShapeDtypeStruct((STEPS, columns), F32),
        ),
        in_specs=[pl.BlockSpec(memory_space=pl.ANY)] * 6,
        out_specs=(pl.BlockSpec(memory_space=vmem), pl.BlockSpec(memory_space=vmem)),
        scratch_shapes=[
            vmem((leaves, size, columns), F32),
            vmem((leaves, size, columns), F32),
            vmem((2, leaves, size, size), BF16),
            vmem((2, leaves, 2, size, rank), BF16),
            vmem((2, nodes, 3, rank, rank), BF16),
            vmem((2, heights, 3, rank, rank), BF16),
            vmem((2, 2, rank, rank), BF16),
            vmem((2, leaves, rank, size), BF16),
            vmem((2, leaves - 1, rank, 2 * rank), BF16),
            vmem((2, levels, rank, 2 * rank), BF16),
            vmem((2, 2 * rank, leaves * rank), BF16),
            vmem((2, 2 * leaves * rank, rank), BF16),
            vmem((nodes - 1, rank, 2 * columns), BF16),
            vmem((nodes - 1, rank, columns), F32),
            vmem((STEPS + 1, 8, columns), F32),
            vmem((2, group, cut + 8, rank), F32),
            vmem((2, group, cut + 8, rank), F32),
            vmem((2, levels, cut + 8, rank), F32),
            vmem((2, levels, cut, rank), F32),
            vmem((2, levels, cut + 8, rank), F32),
            vmem((2, levels, cut, rank), F32),
            vmem((2, columns, rank), F32),
            vmem((2, bits, half, rank), F32),
            vmem((2, bits, half, rank), F32),
            vmem((2, bits, half, rank), F32),
            vmem((2, bits, half, rank), F32),
            vmem((2, 3, rank, columns), F32),
            vmem((2, columns, rank), F32),
            pltpu.SemaphoreType.DMA((12,)),
            pltpu.SemaphoreType.DMA((2, copies)),
            pltpu.SemaphoreType.DMA((2, copies)),
        ],
        compiler_params=pltpu.CompilerParams(
            collective_id=0, has_side_effects=True, vmem_limit_bytes=48 * 1024 * 1024
        ),
    )(
        right_sides.reshape(leaves, size, columns),
        near_blocks,
        leaf_bases,
        local_factors,
        upper_factors,
        top_couplings,
    )
    return out.reshape(-1, columns), norms


def solution(mesh):
    placed = (
        P(("rows", "leaf"), None),
        P(None, ("rows", "leaf"), None, None),
        P(None, ("rows", "leaf"), None, None, None),
        P(None, ("rows", "leaf"), None, None, None),
        P(None, ("rows", "leaf"), None, None, None, None),
        P(),
    )
    return jax.shard_map(
        body,
        mesh=mesh,
        in_specs=placed,
        out_specs=(P(("rows", "leaf"), None), P()),
        check_vma=False,
    )
```

```python
import functools
import jax
import jax.numpy as jnp
from jax import lax
from jax.experimental import pallas as pl
from jax.experimental.pallas import tpu as pltpu
from jax.sharding import PartitionSpec as P

STEPS = 3
F32 = jnp.float32
BF16 = jnp.bfloat16
NT = (((1,), (1,)), ((), ()))


def dot(a, b):
    return jnp.dot(a, b, preferred_element_type=F32)


def split(v):
    hi = v.astype(BF16)
    lo = (v - hi.astype(F32)).astype(BF16)
    return hi, lo


def wide(v):
    return jnp.concatenate(split(v), axis=1)


def tall(v):
    return jnp.concatenate(split(v), axis=0)


def fold_cols(v):
    n = v.shape[1] // 2
    return v[:, :n] + v[:, n:]


def fold_rows(v):
    n = v.shape[0] // 2
    return v[:n] + v[n:]


def combine(out):
    n, m = out.shape[0] // 2, out.shape[1] // 2
    return out[:n, :m] + (out[:n, m:] + out[n:, :m])


def group_bits(levels):
    return min(3, levels - 2)


def kernel(
    bits_leaf, bits_rows,
    rhs_hbm, near_hbm, bases_hbm, local_hbm, upper_hbm, top_hbm,
    x_ref, norm_ref,
    b_ref, r_ref, near, bases, local, upper, top,
    vt, pt, tt, et, jt, cb, pre, nrm,
    w_send, w_recv, high_a, high_b, got_a, got_b, plane,
    send_a, send_b, recv_a, recv_b, sib_full, full,
    load_sem, send_sem, recv_sem,
):
    leaves = near.shape[1]
    levels = bits_leaf + bits_rows
    last = levels - 1
    bits = group_bits(levels)
    group = 2**bits
    root = 2 * leaves - 2
    leaf = lax.axis_index("leaf")
    rows = lax.axis_index("rows")
    columns = x_ref.shape[2]
    half = columns // 2
    cut = columns // group
    mine = pl.multiple_of(leaf % 2 * half, half)
    other = pl.multiple_of((1 - leaf % 2) * half, half)
    top_pos = rows // 2 ** (bits_rows - 1)

    def flipped(value, mask):
        for bit in range(mask.bit_length()):
            d = 2**bit
            if mask & d:
                value = value + d - 2 * d * (value // d % 2)
        return value

    def device(mask):
        leaf_mask = mask % 2**bits_leaf
        return (flipped(rows, mask // 2**bits_leaf), flipped(leaf, leaf_mask))

    def member(place):
        row, column = place
        if bits <= bits_leaf:
            return column % group
        return column + 2**bits_leaf * (row % 2 ** (bits - bits_leaf))

    me = member((rows, leaf))
    my_rows = pl.multiple_of(me * cut, cut)

    def load(src, dst, index):
        return pltpu.make_async_copy(src, dst, load_sem.at[index])

    loads = {}
    order = []
    for s in (1, 0):
        order += [
            (("local", s), local_hbm.at[s], local.at[s]),
            (("upper", s), upper_hbm.at[s, 0], upper.at[s]),
            (("bases", s), bases_hbm.at[s], bases.at[s]),
        ]
        if s == 1:
            order += [("res", rhs_hbm, r_ref)]
        order += [
            (("near", s), near_hbm.at[s], near.at[s]),
            (("top", s), top_hbm.at[s], top.at[s]),
        ]
        if s == 1:
            order += [("rhs", rhs_hbm, b_ref)]
    for index, (name, src, dst) in enumerate(order):
        loads[name] = load(src, dst, index)
        loads[name].start()

    barrier = pltpu.get_barrier_semaphore()
    partners = list(range(1, group)) + [2**level for level in range(bits, levels)]
    partners.append(2**last + 2 ** (last - 1))
    for mask in partners:
        pl.semaphore_signal(
            barrier, inc=1, device_id=device(mask), device_id_type=pl.DeviceIdType.MESH
        )

    def chain(s, which):
        product = upper[s, bits - 2, which].astype(F32)
        for index in range(bits - 3, -1, -1):
            product = fold_cols(dot(upper[s, index, which], wide(product)))
        node = {root: fold_cols(dot(local[s, root, which], wide(product)))}
        for n in range(root - 1, -1, -1):
            parent = leaves + n // 2
            node[n] = fold_cols(dot(local[s, n, which], wide(node[parent])))
        return [node[i] for i in range(leaves)]

    def setup_chain(s):
        loads["local", s].wait()
        loads["upper", s].wait()
        et[s] = tall(jnp.concatenate([v.T for v in chain(s, 0)], axis=1))

    def setup_up(s):
        loads["bases", s].wait()
        for i in range(leaves):
            vt[s, i] = bases[s, i, 1].astype(F32).T.astype(BF16)

    def setup_pairs(s):
        for p in range(leaves - 1):
            pair = [local[s, 2 * p + j, 0].astype(F32).T.astype(BF16) for j in range(2)]
            pt[s, p] = jnp.concatenate(pair, axis=1)

    def setup_couplings(s):
        loads["top", s].wait()
        for first, stop in ((1, bits), (bits, levels)):
            product = None
            for level in range(first, stop):
                coupling = top[s, top_pos] if level == last else upper[s, level - 1, 2]
                if product is None:
                    value = coupling.astype(F32)
                else:
                    value = fold_rows(dot(tall(product), coupling))
                tt[s, level] = wide(value.T)
                if level + 1 < stop:
                    q = upper[s, level - 1, 1]
                    product = q.astype(F32) if product is None else fold_rows(dot(tall(product), q))

    def setup_down(s):
        jt[s] = tall(jnp.concatenate(chain(s, 1), axis=0))

    def across(s, value, level):
        return combine(dot(tall(value), tt[s, level]))

    def apply(s, norms, hooks):
        started = []
        counter = [0]

        def start(src, dst, mask):
            index = counter[0]
            counter[0] += 1
            copy = pltpu.make_async_remote_copy(
                src_ref=src,
                dst_ref=dst,
                send_sem=send_sem.at[s, index],
                recv_sem=recv_sem.at[s, index],
                device_id=device(mask),
                device_id_type=pl.DeviceIdType.MESH,
            )
            copy.start()
            started.append(copy)
            return copy

        def pieces(i):
            return wide(x_ref[i]) if s == 0 else r_ref[i].astype(BF16)

        def fold(v):
            return fold_cols(v) if s == 0 else v

        def near_leaf(i):
            value = fold(dot(near[s, i], pieces(i)))
            if s == 0:
                r_ref[i] = b_ref[i] - value
            else:
                x_ref[i] = x_ref[i] + value

        def couple(n):
            sibling = n + 1 - 2 * (n % 2)
            pre[n] = fold_cols(dot(local[s, n, 2], cb[sibling]))

        field = {}

        def inner():
            for p in range(leaves - 1):
                stacked = jnp.concatenate([cb[2 * p], cb[2 * p + 1]], axis=0)
                coefficient = fold_cols(dot(pt[s, p], stacked))
                if p < leaves - 2:
                    cb[leaves + p] = wide(coefficient)
            full[s] = fold_rows(dot(tall(coefficient.T), local[s, root, 0]))
            sib_full[s, 0] = coefficient
            copy_a = start(full.at[s, pl.ds(other, half)], recv_a.at[s, 0], 1)
            copies_b = [start(sib_full.at[s, 0], sib_full.at[s, 1], 1)]
            yield
            for level in range(1, bits):
                copy_a.wait_recv()
                if level == 1:
                    value = full[s, pl.ds(mine, half)] + recv_a[s, 0]
                else:
                    value = send_a[s, level - 1] + recv_a[s, level - 1]
                if level < bits - 1:
                    send_a[s, level] = fold_rows(dot(tall(value), upper[s, level - 1, 0]))
                    copy_a = start(send_a.at[s, level], recv_a.at[s, level], 2**level)
                send_b[s, level] = value
                copies_b.append(start(send_b.at[s, level], recv_b.at[s, level], 2**level))
                if level == 1:
                    for n in range(root):
                        couple(n)
                    copies_b[0].wait_recv()
                    root_pre = fold_cols(dot(local[s, root, 2], wide(sib_full[s, 1])))
                yield
            far = None
            for level in range(1, bits):
                copies_b[level].wait_recv()
                term = across(s, recv_b[s, level], level)
                far = term if far is None else far + term
            sib_full[s, 2, pl.ds(mine, half)] = far
            copy = start(
                sib_full.at[s, 2, pl.ds(mine, half)], sib_full.at[s, 2, pl.ds(mine, half)], 1
            )
            yield
            copy.wait_recv()
            far_t = tall(sib_full[s, 2])
            product = lax.dot_general(local[s, root, 1], far_t, NT, preferred_element_type=F32)
            field[root] = fold_cols(product) + root_pre
            for n in range(root - 1, -1, -1):
                parent = leaves + n // 2
                field[n] = fold_cols(dot(local[s, n, 1], wide(field[parent]))) + pre[n]
            yield

        for i in range(leaves):
            cb[i] = wide(fold(dot(vt[s, i], pieces(i))))
        stacked = jnp.concatenate([cb[i] for i in range(leaves)], axis=0)
        outer_t = combine(dot(et[s], stacked)).T
        size = cut if norms is None else cut + 8
        for j in range(group):
            w_send[s, j, :cut] = outer_t[j * cut : (j + 1) * cut]
            if norms is not None:
                w_send[s, j, cut:] = nrm[0]
        copies_w = []
        for e in range(group - 1, 0, -1):
            copies_w.append(
                start(
                    w_send.at[s, member(device(e)), pl.ds(0, size)],
                    w_recv.at[s, e, pl.ds(0, size)],
                    e,
                )
            )
        steps = inner()
        work = list(range(leaves))
        hooks = list(hooks)

        def fill(everything=False):
            if hooks:
                hooks.pop(0)()
            next(steps, None)
            while work:
                near_leaf(work.pop(0))
                if not everything:
                    break

        fill()
        fill()
        for copy in copies_w:
            copy.wait_recv()
        value = w_send[s, me, pl.ds(0, size)]
        for e in range(1, group):
            value = value + w_recv[s, e, pl.ds(0, size)]
        far = None
        for level in range(bits, last - 1):
            coefficient = value[:cut]
            high_a[s, level, :cut] = fold_rows(dot(tall(coefficient), upper[s, level - 1, 0]))
            if norms is not None:
                high_a[s, level, cut:] = value[cut:]
            copy_a = start(
                high_a.at[s, level, pl.ds(0, size)], got_a.at[s, level, pl.ds(0, size)], 2**level
            )
            high_b[s, level] = coefficient
            copy_b = start(high_b.at[s, level], got_b.at[s, level], 2**level)
            fill()
            copy_a.wait_recv()
            value = high_a[s, level, pl.ds(0, size)] + got_a[s, level, pl.ds(0, size)]
            copy_b.wait_recv()
            term = across(s, got_b[s, level], level)
            far = term if far is None else far + term
        low, high = last - 1, last
        coefficient = value[:cut]
        high_a[s, high, :cut] = fold_rows(dot(tall(coefficient), upper[s, low - 1, 0]))
        high_a[s, low, :cut] = coefficient
        if norms is not None:
            high_a[s, high, cut:] = value[cut:]
            high_a[s, low, cut:] = value[cut:]
        copies_top = [
            start(high_a.at[s, src, pl.ds(0, size)], got_a.at[s, dst, pl.ds(0, size)], mask)
            for src, dst, mask in (
                (high, high + 1, 2**high + 2**low),
                (high, high, 2**high),
                (low, low, 2**low),
            )
        ]
        fill()
        copies_top[2].wait_recv()
        got = got_a[s, low, pl.ds(0, size)]
        if norms is not None:
            value = value + got
        term = across(s, got[:cut], low)
        far = term if far is None else far + term
        fill(True)
        while hooks:
            hooks.pop(0)()
        copies_top[1].wait_recv()
        copies_top[0].wait_recv()
        got = got_a[s, high, pl.ds(0, size)] + got_a[s, high + 1, pl.ds(0, size)]
        if norms is not None:
            nrm[norms] = value[cut:] + got[cut:]
        far = far + across(s, got[:cut], high)
        plane[s, pl.ds(my_rows, cut)] = far
        copies_f = []
        for e in range(group - 1, 0, -1):
            piece = plane.at[s, pl.ds(my_rows, cut)]
            copies_f.append(start(piece, piece, e))
        for _ in steps:
            pass
        for copy in copies_f:
            copy.wait_recv()
        outer = combine(
            lax.dot_general(jt[s], tall(plane[s]), NT, preferred_element_type=F32)
        )
        rank = plane.shape[2]
        partial = None
        for i in range(leaves):
            total = field[i] + outer[i * rank : (i + 1) * rank]
            if s == 0:
                out = r_ref[i] - fold_cols(dot(bases[s, i, 0], wide(total)))
                r_ref[i] = out
                square = jnp.sum((out * out).reshape(-1, 8, out.shape[1]), axis=0)
                partial = square if partial is None else partial + square
            else:
                x_ref[i] = x_ref[i] + dot(bases[s, i, 0], total.astype(BF16))
        if s == 0:
            nrm[0] = partial
        for copy in started:
            copy.wait_send()

    setup_chain(1)
    setup_up(1)
    x_ref[...] = jnp.zeros(x_ref.shape, F32)
    loads["res"].wait()
    pl.semaphore_wait(barrier, len(partners))

    def first():
        setup_pairs(1)
        loads["near", 1].wait()

    def second():
        setup_couplings(1)
        setup_down(1)

    def third():
        setup_chain(0)
        setup_up(0)
        setup_pairs(0)

    def fourth():
        setup_couplings(0)
        setup_down(0)
        loads["near", 0].wait()
        loads["rhs"].wait()

    apply(1, None, [first, second, third, fourth])

    def step(k, carry):
        apply(0, None, [])
        apply(1, k + 1, [])
        return carry

    lax.fori_loop(0, STEPS, step, 0)
    for k in range(STEPS):
        norm_ref[pl.ds(k, 1)] = jnp.sum(nrm[k + 1], axis=0, keepdims=True)


def body(right_sides, near_blocks, leaf_bases, local_factors, upper_factors, top_couplings):
    bits_leaf = lax.axis_size("leaf").bit_length() - 1
    bits_rows = lax.axis_size("rows").bit_length() - 1
    levels = bits_leaf + bits_rows
    leaves, size = near_blocks.shape[1], near_blocks.shape[2]
    rank = leaf_bases.shape[4]
    columns = right_sides.shape[1]
    half = columns // 2
    bits = group_bits(levels)
    group = 2**bits
    cut = columns // group
    copies = 2 * (group - 1) + 2 * levels
    nodes = local_factors.shape[1]
    heights = upper_factors.shape[2]
    vmem = pltpu.VMEM
    out, norms = pl.pallas_call(
        functools.partial(kernel, bits_leaf, bits_rows),
        out_shape=(
            jax.ShapeDtypeStruct((leaves, size, columns), F32),
            jax.ShapeDtypeStruct((STEPS, columns), F32),
        ),
        in_specs=[pl.BlockSpec(memory_space=pl.ANY)] * 6,
        out_specs=(pl.BlockSpec(memory_space=vmem), pl.BlockSpec(memory_space=vmem)),
        scratch_shapes=[
            vmem((leaves, size, columns), F32),
            vmem((leaves, size, columns), F32),
            vmem((2, leaves, size, size), BF16),
            vmem((2, leaves, 2, size, rank), BF16),
            vmem((2, nodes, 3, rank, rank), BF16),
            vmem((2, heights, 3, rank, rank), BF16),
            vmem((2, 2, rank, rank), BF16),
            vmem((2, leaves, rank, size), BF16),
            vmem((2, leaves - 1, rank, 2 * rank), BF16),
            vmem((2, levels, rank, 2 * rank), BF16),
            vmem((2, 2 * rank, leaves * rank), BF16),
            vmem((2, 2 * leaves * rank, rank), BF16),
            vmem((nodes - 1, rank, 2 * columns), BF16),
            vmem((nodes - 1, rank, columns), F32),
            vmem((STEPS + 1, 8, columns), F32),
            vmem((2, group, cut + 8, rank), F32),
            vmem((2, group, cut + 8, rank), F32),
            vmem((2, levels, cut + 8, rank), F32),
            vmem((2, levels, cut, rank), F32),
            vmem((2, levels + 1, cut + 8, rank), F32),
            vmem((2, levels, cut, rank), F32),
            vmem((2, columns, rank), F32),
            vmem((2, bits, half, rank), F32),
            vmem((2, bits, half, rank), F32),
            vmem((2, bits, half, rank), F32),
            vmem((2, bits, half, rank), F32),
            vmem((2, 3, rank, columns), F32),
            vmem((2, columns, rank), F32),
            pltpu.SemaphoreType.DMA((12,)),
            pltpu.SemaphoreType.DMA((2, copies)),
            pltpu.SemaphoreType.DMA((2, copies)),
        ],
        compiler_params=pltpu.CompilerParams(
            collective_id=0, has_side_effects=True, vmem_limit_bytes=67043328
        ),
    )(
        right_sides.reshape(leaves, size, columns),
        near_blocks,
        leaf_bases,
        local_factors,
        upper_factors,
        top_couplings,
    )
    return out.reshape(-1, columns), norms


def solution(mesh):
    placed = (
        P(("rows", "leaf"), None),
        P(None, ("rows", "leaf"), None, None),
        P(None, ("rows", "leaf"), None, None, None),
        P(None, ("rows", "leaf"), None, None, None),
        P(None, ("rows", "leaf"), None, None, None, None),
        P(),
    )
    return jax.shard_map(
        body,
        mesh=mesh,
        in_specs=placed,
        out_specs=(P(("rows", "leaf"), None), P()),
        check_vma=False,
    )
```
